32 devices in a mesh: group: 2 (over y), fsdp: 16 (over z, x, core).
Axes of the slice: x: 2, y: 2, z: 4, core: 2. Of those that a mesh axis runs over, the one named last changes fastest.
Arguments:
- acts: bfloat16 [2, 8192, 8192], P('group', 'fsdp'), may hold values from -6 to 6
- cotangent: bfloat16 [2, 8192, 512], P('group', 'fsdp'), may hold values from -5.40625 to 5.40625
- inner_params: float32 [2, 8192, 512], P('group', 'fsdp'), may hold values from -6 to 6
- adam_first: float32 [2, 8192, 512], P('group', 'fsdp'), may hold values from -0.018 to 0.018
- adam_second: float32 [2, 8192, 512], P('group', 'fsdp'), may hold values from 1e-06 to 0.0001
- inner_steps: int32 [2], replicated, may hold values from 8 to 128
- group_tokens: int32 [2], replicated, may hold values from 16384 to 131072
- anchor: float32 [8192, 512], P(('fsdp', 'group')), may hold values from -6 to 6
- momentum: float32 [8192, 512], P(('fsdp', 'group')), may hold values from -2 to 2
Outputs:
- new_anchor: float32 [8192, 512], P(('fsdp', 'group'))
- new_momentum: float32 [8192, 512], P(('fsdp', 'group'))
- group_weights: bfloat16 [2, 8192, 512], P('group', 'fsdp')
The draws below stay inside these ranges and needn't reach their ends.
All inputs are finite; a program needn't handle non-finite values.
Results may differ from the reference program's by a relative error of at most 0.0004.
Values may be sent and summed in bfloat16 or wider, within the bound.
A program may use at most 128 MiB of HBM per device.

```python
import math
import jax
import jax.numpy as jnp

D = 8192
KV = 512
TOK_DEV = 512
TOKG = 8192
N_GROUP = 2
N_FSDP = 16


def strengthened(values, rng, source, target, blocks, factor):
    def block_of(position):
        return (jnp.arange(values.shape[position]) // (values.shape[position] // blocks)).reshape((-1,) + (1,) * (values.ndim - 1 - position))

    first = jax.random.permutation(rng, blocks)[block_of(target)]
    far = (block_of(target) + blocks // 2) % blocks
    return jnp.where((block_of(source) == first) | (block_of(source) == far), factor * values, values)


def shard_levels(key, shape, pieces, low, high):
    def one(position, shards_of):
        heights = jax.random.uniform(jax.random.fold_in(jax.random.fold_in(key, 6), position), (shards_of,), jnp.float32, low / len(pieces), high / len(pieces))
        return jnp.repeat(jnp.exp(heights), shape[position] // shards_of).reshape((-1,) + (1,) * (len(shape) - position - 1))

    gain = one(*pieces[0])
    for cut in pieces[1:]:
        gain = gain * one(*cut)
    return gain


def normal_values(key, shape, deviation, bound, shards=(), held_as=jnp.bfloat16):
    values = jax.random.normal(key, shape, jnp.float32) * deviation
    if len(shards) > 0:
        values = shard_levels(key, shape, shards, -0.22, 0.18) * values
    return jnp.clip(values, min=-bound, max=bound).astype(held_as)


def gaussian_with(own_key, extent, deviation, bound, shards, heavy, kind=jnp.bfloat16):
    array = deviation * jax.random.normal(own_key, extent, jnp.float32)
    if shards:
        array = array * shard_levels(own_key, extent, shards, -0.22, 0.18)
    return jnp.clip(strengthened(array, jax.random.fold_in(own_key, 3), *heavy), -bound, bound).astype(kind)


def setup_inputs(seed: int = 0) -> dict:
    seeds = jax.random.split(jax.random.key(seed), 10)
    return {
        "acts": gaussian_with(seeds[0], (N_GROUP, TOKG, D), 1.0, 6.0, ((0, 2), (1, 16)), (1, 2, 16, 2.0)),
        "cotangent": normal_values(seeds[1], (N_GROUP, TOKG, KV), (0.01 * TOKG ** 0.5), 5.40625, ((0, 2), (1, 16))),
        "inner_params": normal_values(seeds[2], (N_GROUP, D, KV), 1.0, 6.0, ((0, 2), (1, 16)), jnp.float32),
        "adam_first": normal_values(seeds[3], (N_GROUP, D, KV), 0.003, 0.018, ((0, 2), (1, 16)), jnp.float32),
        "adam_second": jnp.clip(jnp.exp(math.log(0.0001) - 4.6051702 * jax.random.uniform(seeds[4], (N_GROUP, D, KV), jnp.float32) ** shard_levels(seeds[4], (N_GROUP, D, KV), ((0, 2), (1, 16)), -0.2, 0.2)), 9.999999974752427e-07, 0.0001),
        "inner_steps": jax.random.randint(seeds[5], (N_GROUP,), 8, 129).astype(jnp.int32),
        "group_tokens": jax.random.randint(seeds[6], (N_GROUP,), 16384, 131073).astype(jnp.int32),
        "anchor": normal_values(seeds[7], (D, KV), 1.0, 6.0, ((0, 32),), jnp.float32),
        "momentum": normal_values(seeds[8], (D, KV), 0.3, 2.0, ((0, 32),), jnp.float32),
    }


beta_one = 0.9
beta_two = 0.95
epsilon = 1e-08
inner_rate = 0.3
decay_rate = 0.1
outer_rate = 0.7
outer_mom = 0.9

def inner_update(params, first_moment, second_moment, gradient, steps):
    fresh_first = beta_one * first_moment + (1.0 - beta_one) * gradient
    fresh_second = beta_two * second_moment + (1.0 - beta_two) * gradient * gradient
    steps_float = steps.astype(jnp.float32)
    correct_one = 1.0 - jnp.power(jnp.float32(beta_one), steps_float)
    correct_two = 1.0 - jnp.power(jnp.float32(beta_two), steps_float)
    ratio = fresh_first / correct_one / (jnp.sqrt(fresh_second / correct_two) + epsilon)
    return params - inner_rate * (ratio + decay_rate * params)

def outer_update(anchor, momentum, merged):
    pseudo = anchor - merged
    fresh_momentum = outer_mom * momentum + pseudo
    fresh_anchor = anchor - outer_rate * (pseudo + outer_mom * fresh_momentum)
    return (fresh_anchor, fresh_momentum)

def reference(acts, cotangent, inner_params, adam_first, adam_second, inner_steps, group_tokens, anchor, momentum):
    counts = group_tokens.astype(jnp.float32)
    shares = counts / jnp.sum(counts)
    merged = jnp.zeros((D, KV), jnp.float32)
    for member in range(N_GROUP):
        gradient = jnp.dot(acts[member].T, cotangent[member], preferred_element_type=jnp.float32) / (TOK_DEV * N_FSDP)
        updated = inner_update(inner_params[member], adam_first[member], adam_second[member], gradient, inner_steps[member])
        merged = merged + shares[member] * updated
    new_anchor, new_momentum = outer_update(anchor, momentum, merged)
    group_weights = jnp.broadcast_to(new_anchor.astype(jnp.bfloat16)[None], (N_GROUP, D, KV))
    return (new_anchor, new_momentum, group_weights)
```

```python
import functools

import jax
import jax.numpy as jnp
from jax import lax
from jax.experimental import pallas as pl
from jax.experimental.pallas import tpu as pltpu
from jax.sharding import PartitionSpec as P

beta_one = 0.9
beta_two = 0.95
epsilon = 1e-08
inner_rate = 0.3
decay_rate = 0.1
outer_rate = 0.7
outer_mom = 0.9


def inner_update(params, first_moment, second_moment, gradient, steps):
    fresh_first = beta_one * first_moment + (1.0 - beta_one) * gradient
    fresh_second = beta_two * second_moment + (1.0 - beta_two) * gradient * gradient
    steps_float = steps.astype(jnp.float32)
    correct_one = 1.0 - jnp.power(jnp.float32(beta_one), steps_float)
    correct_two = 1.0 - jnp.power(jnp.float32(beta_two), steps_float)
    ratio = fresh_first / correct_one / (jnp.sqrt(fresh_second / correct_two) + epsilon)
    return params - inner_rate * (ratio + decay_rate * params)


def outer_update(anchor, momentum, merged):
    pseudo = anchor - merged
    fresh_momentum = outer_mom * momentum + pseudo
    fresh_anchor = anchor - outer_rate * (pseudo + outer_mom * fresh_momentum)
    return (fresh_anchor, fresh_momentum)


def per_device(
    acts,
    cotangent,
    inner_params,
    adam_first,
    adam_second,
    inner_steps,
    group_tokens,
    anchor,
    momentum,
):
    fsdp_count = lax.axis_size("fsdp")
    group_index = lax.axis_index("group")
    inputs = acts[0]
    upstream = cotangent[0]
    group_total = inputs.shape[0] * fsdp_count
    contract = (((0,), (0,)), ((), ()))
    summed = lax.psum_scatter(
        lax.dot_general(inputs, upstream, contract, preferred_element_type=jnp.float32),
        "fsdp",
        scatter_dimension=0,
        tiled=True,
    )
    gradient = summed / group_total
    steps = lax.dynamic_index_in_dim(inner_steps, group_index, 0, False)
    updated = inner_update(inner_params[0], adam_first[0], adam_second[0], gradient, steps)
    counts = group_tokens.astype(jnp.float32)
    share = lax.dynamic_index_in_dim(counts, group_index, 0, False) / jnp.sum(counts)
    weighted = share * updated
    merged = lax.psum_scatter(weighted, "group", scatter_dimension=0, tiled=True)
    new_anchor, new_momentum = outer_update(anchor, momentum, merged)
    rebuilt = lax.all_gather(new_anchor.astype(jnp.bfloat16), "group", axis=0, tiled=True)
    return (new_anchor, new_momentum, rebuilt[None])


MESH = pl.DeviceIdType.MESH
WIRE = jnp.int16
LEVELS = 32767.0
SMALLEST = 1e-30
PIECES = 4
HALVES = 2
FIRST_ORDER = (1, 2, 3)
OTHER_ORDER = (2, 1, 3)
ORDERS = (FIRST_ORDER, OTHER_ORDER, FIRST_ORDER, FIRST_ORDER)
STEPS = 3
PLAN = (
    ("mul", 0, 1), ("mul", 1, 1), ("mul", 2, 1), ("mul", 0, 0), ("mul", 1, 0),
    ("add", 0, 0, 1), ("add", 1, 0, 1), ("add", 0, 1, 1), ("add", 1, 1, 1),
    ("mul", 3, 1), ("mul", 2, 0), ("mul", 3, 0),
    ("add", 0, 0, 2), ("add", 0, 1, 2), ("add", 2, 0, 1), ("add", 0, 0, 3),
    ("add", 2, 0, 2), ("add", 2, 1, 1), ("add", 0, 1, 3), ("add", 1, 0, 2),
    ("add", 2, 1, 2), ("add", 2, 0, 3), ("add", 1, 1, 2), ("add", 1, 0, 3),
    ("add", 2, 1, 3), ("add", 1, 1, 3), ("add", 3, 0, 1), ("add", 3, 0, 2),
    ("add", 3, 1, 1), ("add", 3, 0, 3), ("add", 3, 1, 2), ("add", 3, 1, 3),
)


def outer_step_kernel(
    group_total,
    scalars,
    acts,
    cotangent,
    params_in,
    first_in,
    second_in,
    anchor_in,
    momentum_in,
    anchor_out,
    momentum_out,
    weights_out,
    acts_buf,
    cot_buf,
    cot_t,
    own,
    send1,
    send2,
    send3,
    recv1,
    recv2,
    recv3,
    scale_send,
    scale_recv,
    params,
    first,
    second,
    anchor,
    momentum,
    weighted_send,
    weighted_recv,
    fresh_send,
    fresh_recv,
    local_sem,
    acts_send_sem,
    acts_recv_sem,
    cot_sem,
    state_sem,
    step_send_sem,
    step_recv_sem,
    scale_send_sem,
    scale_recv_sem,
    weighted_send_sem,
    weighted_recv_sem,
    fresh_send_sem,
    fresh_recv_sem,
):
    tokens, _ = acts.shape
    rows, width = params.shape
    cols = rows // PIECES
    half_width = width // HALVES
    half_rows = rows // 2
    me = lax.axis_index("fsdp")
    group = lax.axis_index("group")
    other_group = 1 - group
    bits = [(me // (1 << k)) % 2 for k in range(STEPS + 1)]

    def across(k):
        return (group, me + (1 - 2 * bits[k]) * (1 << k))

    sibling = across(0)
    peer = (other_group, me)
    sends, recvs = (send1, send2, send3), (recv1, recv2, recv3)

    state = []
    for n, (src, dst) in enumerate(
        ((params_in, params), (first_in, first), (second_in, second), (anchor_in, anchor), (momentum_in, momentum))
    ):
        state.append(pltpu.make_async_copy(src, dst, state_sem.at[n]))
    cot_local = pltpu.make_async_copy(cotangent, cot_buf.at[pl.ds(0, tokens)], cot_sem.at[0])
    cot_remote = pltpu.make_async_remote_copy(
        src_ref=cotangent,
        dst_ref=cot_buf.at[pl.ds(tokens, tokens)],
        send_sem=cot_sem.at[1],
        recv_sem=cot_sem.at[2],
        device_id=sibling,
        device_id_type=MESH,
    )

    def column_piece(i):
        return (other_group * (PIECES // 2) + i) % PIECES

    def acts_columns(i, pos, core):
        block = core
        for s, k in enumerate(ORDERS[i]):
            bit = bits[k] if (pos >> (STEPS - 1 - s)) % 2 == 0 else 1 - bits[k]
            block = block + bit * (1 << k)
        return pl.ds(pl.multiple_of(block * rows + column_piece(i) * cols, cols), cols)

    acts_remote = {}
    acts_local = {}
    for i in range(PIECES):
        for pos in range(8):
            acts_local[i, pos] = pltpu.make_async_copy(
                acts.at[:, acts_columns(i, pos, bits[0])],
                acts_buf.at[i, pos, pl.ds(0, tokens)],
                local_sem.at[i, pos],
            )
            acts_remote[i, pos] = pltpu.make_async_remote_copy(
                src_ref=acts.at[:, acts_columns(i, pos, 1 - bits[0])],
                dst_ref=acts_buf.at[i, pos, pl.ds(tokens, tokens)],
                send_sem=acts_send_sem.at[i, pos],
                recv_sem=acts_recv_sem.at[i, pos],
                device_id=sibling,
                device_id_type=MESH,
            )

    barrier = pltpu.get_barrier_semaphore()
    for target in (sibling, across(1), across(2), across(3), peer):
        pl.semaphore_signal(barrier, inc=1, device_id=target, device_id_type=MESH)
    cot_local.start()
    need = [(e[1], e[2]) for e in PLAN if e[0] == "mul"]
    for i, part in need:
        for pos in range(4 * part, 4 * part + 4):
            acts_local[i, pos].start()
    for copy in state:
        copy.start()
    pl.semaphore_wait(barrier, 5)
    cot_remote.start()
    for i, part in need:
        for pos in range(4 * part, 4 * part + 4):
            acts_remote[i, pos].start()

    scale_send[...] = jnp.zeros_like(scale_send)
    cot_local.wait()
    cot_remote.wait_recv()
    cot_t[...] = cot_buf[...].astype(jnp.float32).T.astype(jnp.bfloat16)

    flying = []

    def send_step(i, h, step):
        copy = pltpu.make_async_remote_copy(
            src_ref=sends[step - 1].at[i, h],
            dst_ref=recvs[step - 1].at[i, h],
            send_sem=step_send_sem.at[step - 1, i, h],
            recv_sem=step_recv_sem.at[step - 1, i, h],
            device_id=across(ORDERS[i][step - 1]),
            device_id_type=MESH,
        )
        scale = pltpu.make_async_remote_copy(
            src_ref=scale_send.at[step - 1, i, h],
            dst_ref=scale_recv.at[step - 1, i, h],
            send_sem=scale_send_sem.at[step - 1, i, h],
            recv_sem=scale_recv_sem.at[step - 1, i, h],
            device_id=across(ORDERS[i][step - 1]),
            device_id_type=MESH,
        )
        scale.start()
        copy.start()
        flying.extend((copy, scale))
        return copy, scale

    def encode(i, h, step, q, value):
        top = jnp.max(jnp.abs(value), axis=0, keepdims=True)
        steps = jnp.where(top > SMALLEST, LEVELS / jnp.maximum(top, SMALLEST), 0.0)
        sends[step - 1][i, h, q] = jnp.round(value * steps).astype(jnp.int32).astype(WIRE)
        scale_send[step - 1, i, h, pl.ds(q, 1)] = top * (1.0 / LEVELS)

    def decode(i, h, step, q):
        coded = recvs[step - 1][i, h, q].astype(jnp.int32).astype(jnp.float32)
        return coded * scale_recv[step - 1, i, h, q : q + 1]

    step_copies = {}

    def multiply(i, part):
        for pos in range(4 * part, 4 * part + 4):
            acts_local[i, pos].wait()
            acts_remote[i, pos].wait_recv()

        @pl.loop(0, 4)
        def _(q):
            product = jnp.dot(cot_t[...], acts_buf[i, 4 * part + q], preferred_element_type=jnp.float32)
            if part == 1:
                for h in range(HALVES):
                    encode(i, h, 1, q, product[h * half_width : (h + 1) * half_width])
            else:
                own[i, q] = product

        if part == 1:
            for h in range(HALVES):
                step_copies[i, h, 1] = send_step(i, h, 1)

    state_waited = []
    one, two, share = scalars[0], scalars[1], scalars[2]

    def finish(i, h, gradient_t):
        if not state_waited:
            for copy in state:
                copy.wait()
            state_waited.append(True)
        lanes = slice(h * half_width, (h + 1) * half_width)
        gradient = gradient_t.T / group_total
        at = pl.ds(pl.multiple_of(column_piece(i) * cols, cols), cols)
        weights = params[at, lanes]
        fresh_first = beta_one * first[at, lanes] + (1.0 - beta_one) * gradient
        fresh_second = beta_two * second[at, lanes] + (1.0 - beta_two) * gradient * gradient
        ratio = fresh_first / one / (jnp.sqrt(fresh_second / two) + epsilon)
        weighted = share * (weights - inner_rate * (ratio + decay_rate * weights))
        if i < PIECES // 2:
            weighted_send[i, h] = weighted
            copy = pltpu.make_async_remote_copy(
                src_ref=weighted_send.at[i, h],
                dst_ref=weighted_recv.at[i, h],
                send_sem=weighted_send_sem.at[i, h],
                recv_sem=weighted_recv_sem.at[i, h],
                device_id=peer,
                device_id_type=MESH,
            )
            copy.start()
            weighted_copies[i, h] = copy
            return
        n = i - PIECES // 2
        weighted_copies[n, h].wait_recv()
        mine = slice(n * cols, (n + 1) * cols)
        new_anchor, new_momentum = outer_update(
            anchor[mine, lanes], momentum[mine, lanes], weighted + weighted_recv[n, h]
        )
        rounded = new_anchor.astype(jnp.bfloat16)
        fresh_send[n, h] = rounded
        copy = pltpu.make_async_remote_copy(
            src_ref=fresh_send.at[n, h],
            dst_ref=fresh_recv.at[n, h],
            send_sem=fresh_send_sem.at[n, h],
            recv_sem=fresh_recv_sem.at[n, h],
            device_id=peer,
            device_id_type=MESH,
        )
        copy.start()
        fresh_copies[n, h] = copy
        anchor_out[mine, lanes] = new_anchor
        momentum_out[mine, lanes] = new_momentum
        at = pl.ds(pl.multiple_of(group * half_rows + n * cols, cols), cols)
        weights_out[at, lanes] = rounded

    weighted_copies = {}
    fresh_copies = {}

    def add(i, h, step):
        for copy in step_copies[i, h, step]:
            copy.wait_recv()
        keys = slice(h * half_width, (h + 1) * half_width)
        held = 8 >> step
        if step == STEPS:
            finish(i, h, own[i, 0, keys] + decode(i, h, step, 0))
            return
        keep = held // 2
        for q in range(keep, held):
            total = own[i, q, keys] + decode(i, h, step, q)
            encode(i, h, step + 1, q - keep, total)
        step_copies[i, h, step + 1] = send_step(i, h, step + 1)
        for q in range(keep):
            own[i, q, keys] += decode(i, h, step, q)

    for event in PLAN:
        if event[0] == "mul":
            multiply(*event[1:])
        else:
            add(*event[1:])

    for n in range(PIECES // 2):
        for h in range(HALVES):
            fresh_copies[n, h].wait_recv()
            at = pl.ds(pl.multiple_of(other_group * half_rows + n * cols, cols), cols)
            weights_out[at, h * half_width : (h + 1) * half_width] = fresh_recv[n, h]
    cot_remote.wait_send()
    for copy in list(acts_remote.values()) + flying + list(weighted_copies.values()) + list(fresh_copies.values()):
        copy.wait_send()


def fused_per_device(
    acts, cotangent, inner_params, adam_first, adam_second, inner_steps, group_tokens, anchor, momentum
):
    group = lax.axis_index("group")
    tokens, _ = acts.shape[1:]
    rows, width = inner_params.shape[1:]
    cols, half_width = rows // PIECES, width // HALVES
    steps = lax.dynamic_index_in_dim(inner_steps, group, 0, False).astype(jnp.float32)
    counts = group_tokens.astype(jnp.float32)
    share = lax.dynamic_index_in_dim(counts, group, 0, False) / jnp.sum(counts)
    scalars = jnp.stack(
        [
            1.0 - jnp.power(jnp.float32(beta_one), steps),
            1.0 - jnp.power(jnp.float32(beta_two), steps),
            share,
        ]
    )
    low, full = jnp.bfloat16, jnp.float32
    dma = pltpu.SemaphoreType.DMA
    stage = [(PIECES, HALVES, 8 >> (s + 1), half_width, cols) for s in range(STEPS)]
    tail = (PIECES // 2, HALVES, cols, half_width)
    new_anchor, new_momentum, weights = pl.pallas_call(
        functools.partial(outer_step_kernel, tokens * lax.axis_size("fsdp")),
        out_shape=(
            jax.ShapeDtypeStruct(anchor.shape, full),
            jax.ShapeDtypeStruct(anchor.shape, full),
            jax.ShapeDtypeStruct((rows, width), low),
        ),
        in_specs=[pl.BlockSpec(memory_space=pltpu.SMEM)] + [pl.BlockSpec(memory_space=pl.ANY)] * 7,
        out_specs=[pl.BlockSpec(memory_space=pltpu.VMEM)] * 3,
        scratch_shapes=[
            pltpu.VMEM((PIECES, 8, 2 * tokens, cols), low),
            pltpu.VMEM((2 * tokens, width), low),
            pltpu.VMEM((width, 2 * tokens), low),
            pltpu.VMEM((PIECES, 4, width, cols), full),
            *[pltpu.VMEM(s, WIRE) for s in stage],
            *[pltpu.VMEM(s, WIRE) for s in stage],
            *[pltpu.VMEM((STEPS, PIECES, HALVES, 8, cols), full)] * 2,
            *[pltpu.VMEM((rows, width), full)] * 3,
            *[pltpu.VMEM((rows // 2, width), full)] * 2,
            pltpu.VMEM(tail, full),
            pltpu.VMEM(tail, full),
            pltpu.VMEM(tail, low),
            pltpu.VMEM(tail, low),
            dma((PIECES, 8)),
            dma((PIECES, 8)),
            dma((PIECES, 8)),
            dma((3,)),
            dma((5,)),
            *[dma((STEPS, PIECES, HALVES))] * 4,
            dma((2, HALVES)),
            dma((2, HALVES)),
            dma((2, HALVES)),
            dma((2, HALVES)),
        ],
        compiler_params=pltpu.CompilerParams(
            collective_id=0, has_side_effects=True, vmem_limit_bytes=48 * 1024 * 1024
        ),
    )(scalars, acts[0], cotangent[0], inner_params[0], adam_first[0], adam_second[0], anchor, momentum)
    return (new_anchor, new_momentum, weights[None])


def choose(*arguments):
    rows = arguments[2].shape[1]
    fits = lax.axis_size("fsdp") == 1 << (STEPS + 1) and lax.axis_size("group") == 2
    if fits and rows % (PIECES * 128) == 0 and arguments[2].shape[2] % (HALVES * 128) == 0:
        return fused_per_device(*arguments)
    return per_device(*arguments)


def solution(mesh):
    placed = (
        P("group", "fsdp", None),
        P("group", "fsdp", None),
        P("group", "fsdp", None),
        P("group", "fsdp", None),
        P("group", "fsdp", None),
        P(),
        P(),
        P(("fsdp", "group"), None),
        P(("fsdp", "group"), None),
    )
    return jax.shard_map(
        choose,
        mesh=mesh,
        in_specs=placed,
        out_specs=(
            P(("fsdp", "group"), None),
            P(("fsdp", "group"), None),
            P("group", "fsdp", None),
        ),
        check_vma=False,
    )
```
